32 devices in a mesh: ta: 8 (over y, x, core), gz: 4 (over z).
Axes of the slice: x: 2, y: 2, z: 4, core: 2. Of those that a mesh axis runs over, the one named last changes fastest.
Arguments:
- source: bfloat16 [8, 4, 2, 4, 3, 12, 256], P('ta', 'gz'), may hold values from -6 to 6
- gauge_field: bfloat16 [8, 4, 4, 2, 3, 3, 256], P('ta', 'gz'), may hold values from -2.5 to 2.5
Outputs:
- twice_applied: bfloat16 [8, 4, 2, 4, 3, 12, 256], P('ta', 'gz')
The draws below stay inside these ranges and needn't reach their ends.
All inputs are finite; a program needn't handle non-finite values.
Results may differ from the reference program's by a relative error of at most 0.0075.
Values may be sent and summed in bfloat16 or wider, within the bound.
A program may use at most 64 MiB of HBM per device.

```python
import jax
import jax.numpy as jnp
from jax import lax

SPINS = 4
COLORS = 3
RHS = 12
NY = 16
NX = 16
NT = 8
NZ = 4
SITES = 256


def steps_of(stream_key, extent, pieces, least, largest):
    factor_of, own = 1.0, jax.random.fold_in(stream_key, 6)
    for axis_at, parts in pieces:
        steps = jnp.exp(jax.random.uniform(jax.random.fold_in(own, axis_at), (parts,), jnp.float32, least / len(pieces), largest / len(pieces)))
        factor_of = factor_of * jnp.repeat(steps, extent[axis_at] // parts).reshape([-1 if axis == axis_at else 1 for axis in range(len(extent))])
    return factor_of


def gaussian(key, dims, spread, reach, pieces=(), kind=jnp.bfloat16):
    gain = steps_of(key, dims, pieces, -0.22, 0.18) if pieces else 1.0
    array = jax.random.normal(key, dims, jnp.float32) * spread * gain
    return jnp.minimum(jnp.maximum(array, -reach), reach).astype(kind)


def setup_inputs(seed: int = 0) -> dict:
    seeds = jax.random.split(jax.random.key(seed), 3)
    source = gaussian(seeds[0], (NT, NZ, 2, SPINS, COLORS, RHS, SITES), 1.0, 6.0, ((0, 8), (1, 4)))
    gauge_field = gaussian(seeds[1], (NT, NZ, 4, 2, COLORS, COLORS, SITES), 0.4, 2.5, ((0, 8), (1, 4)))
    return dict(source=source, gauge_field=gauge_field)


HOPPING = 0.124
GAMMA_PERM = ((3, 2, 1, 0), (3, 2, 1, 0), (2, 3, 0, 1), (2, 3, 0, 1))
GAMMA_PHASE = (((0, 1), (0, 1), (0, -1), (0, -1)),
               ((-1, 0), (1, 0), (1, 0), (-1, 0)),
               ((0, 1), (0, -1), (0, -1), (0, 1)),
               ((1, 0), (1, 0), (1, 0), (1, 0)))


def project(spinor, direction, hop_sign):
    real_part = spinor[..., 0, :, :, :, :].astype(jnp.float32)
    imag_part = spinor[..., 1, :, :, :, :].astype(jnp.float32)
    upper_real = []
    upper_imag = []
    for spin_row in range(2):
        partner = GAMMA_PERM[direction][spin_row]
        phase_re, phase_im = GAMMA_PHASE[direction][spin_row]
        mixed_re = phase_re * real_part[..., partner, :, :, :] - phase_im * imag_part[..., partner, :, :, :]
        mixed_im = phase_re * imag_part[..., partner, :, :, :] + phase_im * real_part[..., partner, :, :, :]
        upper_real.append(real_part[..., spin_row, :, :, :] - hop_sign * mixed_re)
        upper_imag.append(imag_part[..., spin_row, :, :, :] - hop_sign * mixed_im)
    stacked = jnp.stack([jnp.stack(upper_real, -4), jnp.stack(upper_imag, -4)], -5)
    return stacked.astype(jnp.bfloat16)


def color_product(link_field, half_spin, adjoint):
    link_re = link_field[..., 0, :, :, :].astype(jnp.float32)
    link_im = link_field[..., 1, :, :, :].astype(jnp.float32)
    if adjoint:
        link_re = jnp.swapaxes(link_re, -3, -2)
        link_im = -jnp.swapaxes(link_im, -3, -2)
    half_re = half_spin[..., 0, :, :, :, :].astype(jnp.float32)
    half_im = half_spin[..., 1, :, :, :, :].astype(jnp.float32)
    total_re = None
    total_im = None
    for column in range(3):
        mat_re = link_re[..., None, :, column, None, :]
        mat_im = link_im[..., None, :, column, None, :]
        vec_re = half_re[..., :, None, column, :, :]
        vec_im = half_im[..., :, None, column, :, :]
        term_re = mat_re * vec_re - mat_im * vec_im
        term_im = mat_re * vec_im + mat_im * vec_re
        total_re = term_re if total_re is None else total_re + term_re
        total_im = term_im if total_im is None else total_im + term_im
    return jnp.stack([total_re, total_im], -5)


def rebuild(product, direction, hop_sign):
    prod_re = product[..., 0, :, :, :, :]
    prod_im = product[..., 1, :, :, :, :]
    rows_re = [prod_re[..., 0, :, :, :], prod_re[..., 1, :, :, :]]
    rows_im = [prod_im[..., 0, :, :, :], prod_im[..., 1, :, :, :]]
    for spin_row in (2, 3):
        partner = GAMMA_PERM[direction][spin_row]
        phase_re, phase_im = GAMMA_PHASE[direction][spin_row]
        rows_re.append(-hop_sign * (phase_re * prod_re[..., partner, :, :, :] - phase_im * prod_im[..., partner, :, :, :]))
        rows_im.append(-hop_sign * (phase_re * prod_im[..., partner, :, :, :] + phase_im * prod_re[..., partner, :, :, :]))
    return jnp.stack([jnp.stack(rows_re, -4), jnp.stack(rows_im, -4)], -5)


def space_roll(values, direction, amount):
    full_shape = values.shape
    plane_grid = values.reshape(full_shape[:-1] + (NY, NX))
    rolled = jnp.roll(plane_grid, amount, axis=(-1 if direction == 0 else -2))
    return rolled.reshape(full_shape)


def space_hops(spinor, link_all):
    hop_sum = None
    for direction in (0, 1):
        link_field = link_all[..., direction, :, :, :, :]
        ahead_half = space_roll(project(spinor, direction, 1), direction, -1)
        term = rebuild(color_product(link_field, ahead_half, False), direction, 1)
        hop_sum = term if hop_sum is None else hop_sum + term
        behind = color_product(link_field, project(spinor, direction, -1), True)
        hop_sum = hop_sum + rebuild(space_roll(behind, direction, 1), direction, -1)
    return hop_sum


def apply_all(spinor, gauge_field):
    time_count = spinor.shape[0]

    def one_slice(slice_index):
        before_index = (slice_index - 1) % time_count
        after_index = (slice_index + 1) % time_count
        current = spinor[slice_index]
        links_now = gauge_field[slice_index]
        hop_sum = space_hops(current, links_now)
        ahead_half = jnp.roll(project(current, 2, 1), -1, axis=0)
        hop_sum = hop_sum + rebuild(color_product(links_now[:, 2], ahead_half, False), 2, 1)
        behind = jnp.roll(color_product(links_now[:, 2], project(current, 2, -1), True), 1, axis=0)
        hop_sum = hop_sum + rebuild(behind, 2, -1)
        forward_sign = jnp.where(slice_index == time_count - 1, -1.0, 1.0).astype(jnp.float32)
        backward_sign = jnp.where(slice_index == 0, -1.0, 1.0).astype(jnp.float32)
        ahead_time = project(spinor[after_index], 3, 1)
        hop_sum = hop_sum + rebuild(color_product(links_now[:, 3], ahead_time, False) * forward_sign, 3, 1)
        links_before = gauge_field[before_index][:, 3]
        behind_time = color_product(links_before, project(spinor[before_index], 3, -1), True) * backward_sign
        hop_sum = hop_sum + rebuild(behind_time, 3, -1)
        return (current.astype(jnp.float32) - HOPPING * hop_sum).astype(jnp.bfloat16)

    return lax.map(one_slice, jnp.arange(time_count, dtype=jnp.int32))


def reference(source, gauge_field):
    first_pass = apply_all(source, gauge_field)
    return apply_all(first_pass, gauge_field)
```

```python
import functools

import jax
import jax.numpy as jnp
from jax import lax
from jax.experimental import pallas as pl
from jax.experimental.pallas import tpu as pltpu
from jax.sharding import PartitionSpec as P

NX = 16
HOPPING = 0.124
GAMMA_PERM = ((3, 2, 1, 0), (3, 2, 1, 0), (2, 3, 0, 1), (2, 3, 0, 1))
GAMMA_PHASE = (
    ((0, 1), (0, 1), (0, -1), (0, -1)),
    ((-1, 0), (1, 0), (1, 0), (-1, 0)),
    ((0, 1), (0, -1), (0, -1), (0, 1)),
    ((1, 0), (1, 0), (1, 0), (1, 0)),
)
LANES = 128
MESH = pl.DeviceIdType.MESH

HALOS = ((3, 1), (3, -1), (2, 1), (2, -1))


def signed_sum(base, term, sign):
    return base + term if sign > 0 else base - term


def rounded(first, second):
    return jnp.concatenate([first, second], 0).astype(jnp.bfloat16)


def project(psi, direction, hop_sign):
    out = []
    for s in range(2):
        partner = GAMMA_PERM[direction][s]
        pr, pi = GAMMA_PHASE[direction][s]
        row = []
        for c in range(3):
            if pi == 0:
                re = signed_sum(psi(0, s, c), psi(0, partner, c), -hop_sign * pr)
                im = signed_sum(psi(1, s, c), psi(1, partner, c), -hop_sign * pr)
            else:
                re = signed_sum(psi(0, s, c), psi(1, partner, c), hop_sign * pi)
                im = signed_sum(psi(1, s, c), psi(0, partner, c), -hop_sign * pi)
            row.append(rounded(re, im))
        out.append(row)
    return out


def widened(pair):
    wide = pair.astype(jnp.float32)
    return wide[:8], wide[8:]


def shift_sites(tile, direction, steps):
    lane = lax.broadcasted_iota(jnp.int32, (8, LANES), 1)
    if direction == 0:
        column = lane % NX
        if steps > 0:
            return jnp.where(
                column == NX - 1,
                pltpu.roll(tile, NX - 1, axis=1),
                pltpu.roll(tile, LANES - 1, axis=1),
            )
        return jnp.where(
            column == 0,
            pltpu.roll(tile, LANES - (NX - 1), axis=1),
            pltpu.roll(tile, 1, axis=1),
        )
    if steps > 0:
        near = pltpu.roll(tile, LANES - NX, axis=1)
        return jnp.where(lane >= LANES - NX, pltpu.roll(near, 4, axis=0), near)
    near = pltpu.roll(tile, NX, axis=1)
    return jnp.where(lane < NX, pltpu.roll(near, 4, axis=0), near)


def add_hop(acc, half, link, direction, hop_sign):
    for r in range(3):
        lr = [link(0, r, c) for c in range(3)]
        li = [link(1, r, c) for c in range(3)]
        k = []
        for s in range(2):
            re = im = None
            for c in range(3):
                hr, hi = half[s][c]
                tr = lr[c] * hr - li[c] * hi
                ti = lr[c] * hi + li[c] * hr
                re = tr if re is None else re + tr
                im = ti if im is None else im + ti
            k.append((re, im))
            acc[0][s][r] = acc[0][s][r] + re
            acc[1][s][r] = acc[1][s][r] + im
        for s in (2, 3):
            kr, ki = k[GAMMA_PERM[direction][s]]
            pr, pi = GAMMA_PHASE[direction][s]
            if pi == 0:
                acc[0][s][r] = signed_sum(acc[0][s][r], kr, -hop_sign * pr)
                acc[1][s][r] = signed_sum(acc[1][s][r], ki, -hop_sign * pr)
            else:
                acc[0][s][r] = signed_sum(acc[0][s][r], ki, hop_sign * pi)
                acc[1][s][r] = signed_sum(acc[1][s][r], kr, -hop_sign * pi)


def plane(ri, s, c):
    return (ri * 4 + s) * 3 + c


def link_slot(direction, hop_sign):
    return direction * 2 + (0 if hop_sign > 0 else 1)


def kernel(
    groups, source, gauge, out, psi, acc, links, sent, got, links_t, links_z,
    send_sem, recv_sem, link_send, link_recv,
):
    ta, gz = lax.axis_index("ta"), lax.axis_index("gz")
    nt, nz = lax.axis_size("ta"), lax.axis_size("gz")
    above_t = (lax.rem(ta + 1, nt), gz)
    below_t = (lax.rem(ta + nt - 1, nt), gz)
    above_z = (ta, lax.rem(gz + 1, nz))
    below_z = (ta, lax.rem(gz + nz - 1, nz))
    targets = (below_t, above_t, below_z, above_z)

    barrier = pltpu.get_barrier_semaphore()
    for target in targets:
        pl.semaphore_signal(barrier, inc=1, device_id=target, device_id_type=MESH)

    def halo_copy(step, halo, g):
        return pltpu.make_async_remote_copy(
            src_ref=sent.at[step, halo, g],
            dst_ref=got.at[step, halo, g],
            send_sem=send_sem.at[step, halo, g],
            recv_sem=recv_sem.at[step, halo, g],
            device_id=targets[halo],
            device_id_type=MESH,
        )

    def link_copy(which):
        return pltpu.make_async_remote_copy(
            src_ref=gauge.at[0, 0, 3 - which],
            dst_ref=(links_t, links_z)[which],
            send_sem=link_send.at[which],
            recv_sem=link_recv.at[which],
            device_id=(above_t, above_z)[which],
            device_id_type=MESH,
        )

    def put_halos(step, g, at):
        for halo, (direction, hop_sign) in enumerate(HALOS):
            half = project(at, direction, hop_sign)
            for s in range(2):
                for c in range(3):
                    sent[step, halo, g, pl.ds((s * 3 + c) * 16, 16)] = half[s][c]

    for p in range(24):
        rows = source[0, 0, p // 12, p // 3 % 4, p % 3].astype(jnp.float32)
        for g in range(groups):
            psi[0, g, p] = jnp.concatenate(
                [rows[4 * g : 4 * g + 4, :LANES], rows[4 * g : 4 * g + 4, LANES:]], 0
            )

    def load_psi(step, g):
        return lambda ri, s, c: psi[step, g, plane(ri, s, c)]

    def first_halos(g, carry):
        put_halos(0, g, load_psi(0, g))
        return carry

    lax.fori_loop(0, groups, first_halos, 0)
    pl.semaphore_wait(barrier, 4)
    for which in range(2):
        link_copy(which).start()

    def first_sends(g, carry):
        for halo in range(4):
            halo_copy(0, halo, g).start()
        return carry

    lax.fori_loop(0, groups, first_sends, 0)

    def spread(rows, c, scale):
        row = rows[c : c + 1] * scale
        return jnp.concatenate(
            [
                jnp.broadcast_to(row[:, :LANES], (4, LANES)),
                jnp.broadcast_to(row[:, LANES:], (4, LANES)),
            ],
            0,
        )

    def put_link(direction, hop_sign, ri, r, c, tile):
        if hop_sign > 0:
            links[link_slot(direction, 1), ri * 9 + r * 3 + c] = tile
        else:
            links[link_slot(direction, -1), ri * 9 + c * 3 + r] = tile if ri == 0 else -tile

    forward_scale = jnp.where(ta == nt - 1, HOPPING, -HOPPING).astype(jnp.float32)
    backward_scale = jnp.where(ta == 0, HOPPING, -HOPPING).astype(jnp.float32)
    for direction in range(4):
        scale = forward_scale if direction == 3 else jnp.float32(-HOPPING)
        for ri in range(2):
            for r in range(3):
                rows = gauge[0, 0, direction, ri, r].astype(jnp.float32)
                for c in range(3):
                    tile = spread(rows, c, scale)
                    put_link(direction, 1, ri, r, c, tile)
                    if direction < 2:
                        put_link(direction, -1, ri, r, c, shift_sites(tile, direction, -1))

    def load_link(direction, hop_sign):
        slot = link_slot(direction, hop_sign)
        return lambda ri, r, c: links[slot, ri * 9 + r * 3 + c]

    def load_spinor(at):
        return [[[at(ri, s, c) for c in range(3)] for s in range(4)] for ri in range(2)]

    def plane_hops(step):
        def body(g, carry):
            at = load_psi(step, g)
            total = load_spinor(at)
            for direction in (0, 1):
                for hop_sign in (1, -1):
                    pairs = project(at, direction, hop_sign)
                    half = [
                        [
                            tuple(shift_sites(v, direction, hop_sign) for v in widened(pairs[s][c]))
                            for c in range(3)
                        ]
                        for s in range(2)
                    ]
                    add_hop(total, half, load_link(direction, hop_sign), direction, hop_sign)
            for ri in range(2):
                for s in range(4):
                    for c in range(3):
                        acc[g, plane(ri, s, c)] = total[ri][s][c]
            return carry

        lax.fori_loop(0, groups, body, 0)

    def halo_hops(step):
        def body(g, carry):
            total = load_spinor(lambda ri, s, c: acc[g, plane(ri, s, c)])
            for halo, (direction, hop_sign) in enumerate(HALOS):
                halo_copy(step, halo, g).wait_recv()
                half = [
                    [widened(got[step, halo, g, pl.ds((s * 3 + c) * 16, 16)]) for c in range(3)]
                    for s in range(2)
                ]
                add_hop(total, half, load_link(direction, hop_sign), direction, hop_sign)
            final = {}
            for s in range(4):
                for c in range(3):
                    final[0, s, c], final[1, s, c] = widened(
                        rounded(total[0][s][c], total[1][s][c])
                    )
            for ri in range(2):
                for s in range(4):
                    for c in range(3):
                        psi[1 - step, g, plane(ri, s, c)] = final[ri, s, c]
            if step == 0:
                put_halos(1, g, lambda ri, s, c: final[ri, s, c])
                for halo in range(4):
                    halo_copy(1, halo, g).start()
            return carry

        lax.fori_loop(0, groups, body, 0)

    plane_hops(0)
    for which, scale in ((0, backward_scale), (1, jnp.float32(-HOPPING))):
        link_copy(which).wait_recv()
        for ri in range(2):
            for r in range(3):
                rows = (links_t, links_z)[which][ri, r].astype(jnp.float32)
                for c in range(3):
                    put_link(3 - which, -1, ri, r, c, spread(rows, c, scale))
    halo_hops(0)
    plane_hops(1)
    halo_hops(1)

    for p in range(24):
        rows = [psi[0, g, p] for g in range(groups)]
        low = jnp.concatenate([v[:4] for v in rows], 0)
        high = jnp.concatenate([v[4:] for v in rows], 0)
        out[0, 0, p // 12, p // 3 % 4, p % 3] = jnp.concatenate([low, high], 1).astype(jnp.bfloat16)

    def drain(g, carry):
        for step in range(2):
            for halo in range(4):
                halo_copy(step, halo, g).wait_send()
        return carry

    lax.fori_loop(0, groups, drain, 0)
    for which in range(2):
        link_copy(which).wait_send()


def body(source, gauge_field):
    groups = source.shape[5] // 4
    return pl.pallas_call(
        functools.partial(kernel, groups),
        out_shape=jax.ShapeDtypeStruct(source.shape, source.dtype),
        in_specs=[pl.BlockSpec(memory_space=pltpu.VMEM)] * 2,
        out_specs=pl.BlockSpec(memory_space=pltpu.VMEM),
        scratch_shapes=[
            pltpu.VMEM((2, groups, 24, 8, LANES), jnp.float32),
            pltpu.VMEM((groups, 24, 8, LANES), jnp.float32),
            pltpu.VMEM((8, 18, 8, LANES), jnp.float32),
            pltpu.VMEM((2, 4, groups, 96, LANES), jnp.bfloat16),
            pltpu.VMEM((2, 4, groups, 96, LANES), jnp.bfloat16),
            pltpu.VMEM(gauge_field.shape[3:], jnp.bfloat16),
            pltpu.VMEM(gauge_field.shape[3:], jnp.bfloat16),
            pltpu.SemaphoreType.DMA((2, 4, groups)),
            pltpu.SemaphoreType.DMA((2, 4, groups)),
            pltpu.SemaphoreType.DMA((2,)),
            pltpu.SemaphoreType.DMA((2,)),
        ],
        compiler_params=pltpu.CompilerParams(collective_id=0, has_side_effects=True),
        name="dirac_twice",
    )(source, gauge_field)


def solution(mesh):
    spec = P("ta", "gz", None, None, None, None, None)
    return jax.shard_map(body, mesh=mesh, in_specs=(spec, spec), out_specs=spec, check_vma=False)
```

```python
import functools

import jax
import jax.numpy as jnp
from jax import lax
from jax.experimental import pallas as pl
from jax.experimental.pallas import tpu as pltpu
from jax.sharding import PartitionSpec as P

NX = 16
HOPPING = 0.124
GAMMA_PERM = ((3, 2, 1, 0), (3, 2, 1, 0), (2, 3, 0, 1), (2, 3, 0, 1))
GAMMA_PHASE = (
    ((0, 1), (0, 1), (0, -1), (0, -1)),
    ((-1, 0), (1, 0), (1, 0), (-1, 0)),
    ((0, 1), (0, -1), (0, -1), (0, 1)),
    ((1, 0), (1, 0), (1, 0), (1, 0)),
)
LANES = 128
MESH = pl.DeviceIdType.MESH

HALOS = ((3, 1), (3, -1), (2, 1), (2, -1))


def signed_sum(base, term, sign):
    return base + term if sign > 0 else base - term


def rounded(first, second):
    return jnp.concatenate([first, second], 0).astype(jnp.bfloat16)


def project(psi, direction, hop_sign):
    out = []
    for s in range(2):
        partner = GAMMA_PERM[direction][s]
        pr, pi = GAMMA_PHASE[direction][s]
        row = []
        for c in range(3):
            if pi == 0:
                re = signed_sum(psi(0, s, c), psi(0, partner, c), -hop_sign * pr)
                im = signed_sum(psi(1, s, c), psi(1, partner, c), -hop_sign * pr)
            else:
                re = signed_sum(psi(0, s, c), psi(1, partner, c), hop_sign * pi)
                im = signed_sum(psi(1, s, c), psi(0, partner, c), -hop_sign * pi)
            row.append(rounded(re, im))
        out.append(row)
    return out


def widened(pair):
    wide = pair.astype(jnp.float32)
    return wide[:8], wide[8:]


def shift_sites(tile, direction, steps):
    lane = lax.broadcasted_iota(jnp.int32, (8, LANES), 1)
    if direction == 0:
        column = lane % NX
        if steps > 0:
            return jnp.where(
                column == NX - 1,
                pltpu.roll(tile, NX - 1, axis=1),
                pltpu.roll(tile, LANES - 1, axis=1),
            )
        return jnp.where(
            column == 0,
            pltpu.roll(tile, LANES - (NX - 1), axis=1),
            pltpu.roll(tile, 1, axis=1),
        )
    near = pltpu.roll(tile, LANES - NX if steps > 0 else NX, axis=1)
    first_half = lax.broadcasted_iota(jnp.int32, (8, LANES), 0) % 2 == 0
    other = jnp.where(first_half, pltpu.roll(near, 7, axis=0), pltpu.roll(near, 1, axis=0))
    return jnp.where(lane >= LANES - NX if steps > 0 else lane < NX, other, near)


def add_hop(acc, half, link, direction, hop_sign):
    for r in range(3):
        lr = [link(0, r, c) for c in range(3)]
        li = [link(1, r, c) for c in range(3)]
        k = []
        for s in range(2):
            re = im = None
            for c in range(3):
                hr, hi = half[s][c]
                tr = lr[c] * hr - li[c] * hi
                ti = lr[c] * hi + li[c] * hr
                re = tr if re is None else re + tr
                im = ti if im is None else im + ti
            k.append((re, im))
            acc[0][s][r] = acc[0][s][r] + re
            acc[1][s][r] = acc[1][s][r] + im
        for s in (2, 3):
            kr, ki = k[GAMMA_PERM[direction][s]]
            pr, pi = GAMMA_PHASE[direction][s]
            if pi == 0:
                acc[0][s][r] = signed_sum(acc[0][s][r], kr, -hop_sign * pr)
                acc[1][s][r] = signed_sum(acc[1][s][r], ki, -hop_sign * pr)
            else:
                acc[0][s][r] = signed_sum(acc[0][s][r], ki, hop_sign * pi)
                acc[1][s][r] = signed_sum(acc[1][s][r], kr, -hop_sign * pi)


def plane(ri, s, c):
    return (ri * 4 + s) * 3 + c


def link_slot(direction, hop_sign):
    return direction * 2 + (0 if hop_sign > 0 else 1)


def kernel(
    groups, source_hbm, gauge_hbm, out, source, gauge, wide, psi, acc, links, sent, got,
    links_below, load_sem, send_sem, recv_sem, link_send, link_recv,
):
    ta, gz = lax.axis_index("ta"), lax.axis_index("gz")
    nt, nz = lax.axis_size("ta"), lax.axis_size("gz")
    above_t = (lax.rem(ta + 1, nt), gz)
    below_t = (lax.rem(ta + nt - 1, nt), gz)
    above_z = (ta, lax.rem(gz + 1, nz))
    below_z = (ta, lax.rem(gz + nz - 1, nz))
    targets = (below_t, above_t, below_z, above_z)

    source_load = pltpu.make_async_copy(source_hbm, source, load_sem.at[0])
    gauge_load = pltpu.make_async_copy(gauge_hbm, gauge, load_sem.at[1])
    source_load.start()
    gauge_load.start()
    barrier = pltpu.get_barrier_semaphore()
    for target in targets:
        pl.semaphore_signal(barrier, inc=1, device_id=target, device_id_type=MESH)

    def halo_copy(step, halo, g):
        return pltpu.make_async_remote_copy(
            src_ref=sent.at[step, halo, g],
            dst_ref=got.at[step, halo, g],
            send_sem=send_sem.at[step, halo, g],
            recv_sem=recv_sem.at[step, halo, g],
            device_id=targets[halo],
            device_id_type=MESH,
        )

    def link_copy(which):
        return pltpu.make_async_remote_copy(
            src_ref=gauge_hbm.at[pl.ds(9 * (3 - which), 9)],
            dst_ref=links_below.at[which],
            send_sem=link_send.at[which],
            recv_sem=link_recv.at[which],
            device_id=(above_t, above_z)[which],
            device_id_type=MESH,
        )

    def put_halos(step, g, at):
        for halo, (direction, hop_sign) in enumerate(HALOS):
            half = project(at, direction, hop_sign)
            for s in range(2):
                for c in range(3):
                    sent[step, halo, g, pl.ds((s * 3 + c) * 16, 16)] = half[s][c]

    def rows_of(ri, s, c, g):
        return pl.ds(((ri * 3 + c) * groups + g) * 32 + s, 8, stride=4)

    source_load.wait()
    for p in range(source.shape[0]):
        wide[8 * p : 8 * p + 8] = source[p].astype(jnp.float32)
    for g in range(groups):
        for ri in range(2):
            for s in range(4):
                for c in range(3):
                    psi[0, g, plane(ri, s, c)] = wide[rows_of(ri, s, c, g)]

    def load_psi(step, g):
        return lambda ri, s, c: psi[step, g, plane(ri, s, c)]

    def first_halos(g, carry):
        put_halos(0, g, load_psi(0, g))
        return carry

    lax.fori_loop(0, groups, first_halos, 0)
    pl.semaphore_wait(barrier, 4)
    for which in range(2):
        link_copy(which).start()

    def first_sends(g, carry):
        for halo in range(4):
            halo_copy(0, halo, g).start()
        return carry

    lax.fori_loop(0, groups, first_sends, 0)

    first_half = lax.broadcasted_iota(jnp.int32, (8, LANES), 0) % 2 == 0

    def spread(rows, ri, scale):
        return scale * jnp.where(
            first_half,
            jnp.broadcast_to(rows[ri : ri + 1], (8, LANES)),
            jnp.broadcast_to(rows[2 + ri : 3 + ri], (8, LANES)),
        )

    def put_link(direction, hop_sign, ri, r, c, tile):
        if hop_sign > 0:
            links[link_slot(direction, 1), ri * 9 + r * 3 + c] = tile
        else:
            links[link_slot(direction, -1), ri * 9 + c * 3 + r] = tile if ri == 0 else -tile

    forward_scale = jnp.where(ta == nt - 1, HOPPING, -HOPPING).astype(jnp.float32)
    backward_scale = jnp.where(ta == 0, HOPPING, -HOPPING).astype(jnp.float32)
    gauge_load.wait()
    for direction in range(4):
        scale = forward_scale if direction == 3 else jnp.float32(-HOPPING)
        for r in range(3):
            for c in range(3):
                rows = gauge[direction * 9 + r * 3 + c].astype(jnp.float32)
                for ri in range(2):
                    tile = spread(rows, ri, scale)
                    put_link(direction, 1, ri, r, c, tile)
                    if direction < 2:
                        put_link(direction, -1, ri, r, c, shift_sites(tile, direction, -1))

    def load_link(direction, hop_sign):
        slot = link_slot(direction, hop_sign)
        return lambda ri, r, c: links[slot, ri * 9 + r * 3 + c]

    def load_spinor(at):
        return [[[at(ri, s, c) for c in range(3)] for s in range(4)] for ri in range(2)]

    def plane_hops(step):
        def body(g, carry):
            at = load_psi(step, g)
            total = load_spinor(at)
            for direction in (0, 1):
                for hop_sign in (1, -1):
                    pairs = project(at, direction, hop_sign)
                    half = [
                        [
                            tuple(shift_sites(v, direction, hop_sign) for v in widened(pairs[s][c]))
                            for c in range(3)
                        ]
                        for s in range(2)
                    ]
                    add_hop(total, half, load_link(direction, hop_sign), direction, hop_sign)
            for ri in range(2):
                for s in range(4):
                    for c in range(3):
                        acc[g, plane(ri, s, c)] = total[ri][s][c]
            return carry

        lax.fori_loop(0, groups, body, 0)

    def halo_hops(step):
        def body(g, carry):
            total = load_spinor(lambda ri, s, c: acc[g, plane(ri, s, c)])
            for halo, (direction, hop_sign) in enumerate(HALOS):
                halo_copy(step, halo, g).wait_recv()
                half = [
                    [widened(got[step, halo, g, pl.ds((s * 3 + c) * 16, 16)]) for c in range(3)]
                    for s in range(2)
                ]
                add_hop(total, half, load_link(direction, hop_sign), direction, hop_sign)
            final = {}
            for s in range(4):
                for c in range(3):
                    final[0, s, c], final[1, s, c] = widened(
                        rounded(total[0][s][c], total[1][s][c])
                    )
            for (ri, s, c), tile in final.items():
                if step == 0:
                    psi[1, g, plane(ri, s, c)] = tile
                else:
                    wide[rows_of(ri, s, c, g)] = tile
            if step == 0:
                put_halos(1, g, lambda ri, s, c: final[ri, s, c])
                for halo in range(4):
                    halo_copy(1, halo, g).start()
            else:
                for block in range(6):
                    for p in range(4):
                        at = (block * groups + g) * 4 + p
                        out[at] = wide[pl.ds(8 * at, 8)].astype(jnp.bfloat16)
            return carry

        lax.fori_loop(0, groups, body, 0)

    plane_hops(0)
    for which, scale in ((0, backward_scale), (1, jnp.float32(-HOPPING))):
        link_copy(which).wait_recv()
        for r in range(3):
            for c in range(3):
                rows = links_below[which, r * 3 + c].astype(jnp.float32)
                for ri in range(2):
                    put_link(3 - which, -1, ri, r, c, spread(rows, ri, scale))
    halo_hops(0)
    plane_hops(1)
    halo_hops(1)

    def drain(g, carry):
        for step in range(2):
            for halo in range(4):
                halo_copy(step, halo, g).wait_send()
        return carry

    lax.fori_loop(0, groups, drain, 0)
    for which in range(2):
        link_copy(which).wait_send()


def body(source, gauge_field):
    rhs = source.shape[5]
    groups = rhs // 4
    source_rows = source.reshape(2, 4, 3, rhs, 2, LANES).transpose(0, 2, 3, 4, 1, 5)
    source_rows = source_rows.reshape(6 * rhs, 8, LANES)
    gauge_rows = gauge_field.reshape(4, 2, 3, 3, 2, LANES).transpose(0, 2, 3, 4, 1, 5)
    gauge_rows = gauge_rows.reshape(36, 4, LANES)
    rows = pl.pallas_call(
        functools.partial(kernel, groups),
        out_shape=jax.ShapeDtypeStruct(source_rows.shape, source.dtype),
        in_specs=[pl.BlockSpec(memory_space=pltpu.HBM)] * 2,
        out_specs=pl.BlockSpec(memory_space=pltpu.VMEM),
        scratch_shapes=[
            pltpu.VMEM(source_rows.shape, jnp.bfloat16),
            pltpu.VMEM(gauge_rows.shape, jnp.bfloat16),
            pltpu.VMEM((48 * rhs, LANES), jnp.float32),
            pltpu.VMEM((2, groups, 24, 8, LANES), jnp.float32),
            pltpu.VMEM((groups, 24, 8, LANES), jnp.float32),
            pltpu.VMEM((8, 18, 8, LANES), jnp.float32),
            pltpu.VMEM((2, 4, groups, 96, LANES), jnp.bfloat16),
            pltpu.VMEM((2, 4, groups, 96, LANES), jnp.bfloat16),
            pltpu.VMEM((2, 9, 4, LANES), jnp.bfloat16),
            pltpu.SemaphoreType.DMA((2,)),
            pltpu.SemaphoreType.DMA((2, 4, groups)),
            pltpu.SemaphoreType.DMA((2, 4, groups)),
            pltpu.SemaphoreType.DMA((2,)),
            pltpu.SemaphoreType.DMA((2,)),
        ],
        compiler_params=pltpu.CompilerParams(collective_id=0, has_side_effects=True),
        name="dirac_twice",
    )(source_rows, gauge_rows)
    out = rows.reshape(2, 3, rhs, 2, 4, LANES).transpose(0, 4, 1, 2, 3, 5)
    return out.reshape(source.shape)


def solution(mesh):
    spec = P("ta", "gz", None, None, None, None, None)
    return jax.shard_map(body, mesh=mesh, in_specs=(spec, spec), out_specs=spec, check_vma=False)
```

```python
import functools

import jax
import jax.numpy as jnp
from jax import lax
from jax.experimental import pallas as pl
from jax.experimental.pallas import tpu as pltpu
from jax.sharding import PartitionSpec as P

NX = 16
HOPPING = 0.124
GAMMA_PERM = ((3, 2, 1, 0), (3, 2, 1, 0), (2, 3, 0, 1), (2, 3, 0, 1))
GAMMA_PHASE = (
    ((0, 1), (0, 1), (0, -1), (0, -1)),
    ((-1, 0), (1, 0), (1, 0), (-1, 0)),
    ((0, 1), (0, -1), (0, -1), (0, 1)),
    ((1, 0), (1, 0), (1, 0), (1, 0)),
)
LANES = 128
MESH = pl.DeviceIdType.MESH

HALOS = ((3, 1), (3, -1), (2, 1), (2, -1))


def signed_sum(base, term, sign):
    if not isinstance(sign, int):
        return base + term * sign
    return base + term if sign > 0 else base - term


def rounded(first, second):
    return jnp.concatenate([first, second], 0).astype(jnp.bfloat16)


def project(psi, direction, hop_sign):
    out = []
    for s in range(2):
        partner = GAMMA_PERM[direction][s]
        pr, pi = GAMMA_PHASE[direction][s]
        row = []
        for c in range(3):
            if pi == 0:
                re = signed_sum(psi(0, s, c), psi(0, partner, c), -hop_sign * pr)
                im = signed_sum(psi(1, s, c), psi(1, partner, c), -hop_sign * pr)
            else:
                re = signed_sum(psi(0, s, c), psi(1, partner, c), hop_sign * pi)
                im = signed_sum(psi(1, s, c), psi(0, partner, c), -hop_sign * pi)
            row.append(rounded(re, im))
        out.append(row)
    return out


def widened(pair):
    wide = pair.astype(jnp.float32)
    return wide[:8], wide[8:]


def shift_sites(tile, direction, steps):
    lane = lax.broadcasted_iota(jnp.int32, (8, LANES), 1)
    if direction == 0:
        column = lane % NX
        if steps > 0:
            return jnp.where(
                column == NX - 1,
                pltpu.roll(tile, NX - 1, axis=1),
                pltpu.roll(tile, LANES - 1, axis=1),
            )
        return jnp.where(
            column == 0,
            pltpu.roll(tile, LANES - (NX - 1), axis=1),
            pltpu.roll(tile, 1, axis=1),
        )
    near = pltpu.roll(tile, LANES - NX if steps > 0 else NX, axis=1)
    first_half = lax.broadcasted_iota(jnp.int32, (8, LANES), 0) % 2 == 0
    other = jnp.where(first_half, pltpu.roll(near, 7, axis=0), pltpu.roll(near, 1, axis=0))
    return jnp.where(lane >= LANES - NX if steps > 0 else lane < NX, other, near)


def add_hop(acc, half, link, direction, hop_sign):
    for r in range(3):
        lr = [link(0, r, c) for c in range(3)]
        li = [link(1, r, c) for c in range(3)]
        k = []
        for s in range(2):
            re = im = None
            for c in range(3):
                hr, hi = half[s][c]
                tr = lr[c] * hr - li[c] * hi
                ti = lr[c] * hi + li[c] * hr
                re = tr if re is None else re + tr
                im = ti if im is None else im + ti
            k.append((re, im))
            acc[0][s][r] = acc[0][s][r] + re
            acc[1][s][r] = acc[1][s][r] + im
        for s in (2, 3):
            kr, ki = k[GAMMA_PERM[direction][s]]
            pr, pi = GAMMA_PHASE[direction][s]
            if pi == 0:
                acc[0][s][r] = signed_sum(acc[0][s][r], kr, -hop_sign * pr)
                acc[1][s][r] = signed_sum(acc[1][s][r], ki, -hop_sign * pr)
            else:
                acc[0][s][r] = signed_sum(acc[0][s][r], ki, hop_sign * pi)
                acc[1][s][r] = signed_sum(acc[1][s][r], kr, -hop_sign * pi)


def plane(ri, s, c):
    return (ri * 4 + s) * 3 + c


def link_slot(direction, hop_sign):
    return direction * 2 + (0 if hop_sign > 0 else 1)


def kernel(
    groups, source_hbm, gauge_hbm, out, source, gauge, wide, psi, acc, links, sent, got,
    links_below, load_sem, send_sem, recv_sem, link_send, link_recv,
):
    ta, gz = lax.axis_index("ta"), lax.axis_index("gz")
    nt, nz = lax.axis_size("ta"), lax.axis_size("gz")
    above_t = (lax.rem(ta + 1, nt), gz)
    below_t = (lax.rem(ta + nt - 1, nt), gz)
    above_z = (ta, lax.rem(gz + 1, nz))
    below_z = (ta, lax.rem(gz + nz - 1, nz))
    targets = (below_t, above_t, below_z, above_z)

    source_load = pltpu.make_async_copy(source_hbm, source, load_sem.at[0])
    gauge_load = pltpu.make_async_copy(gauge_hbm, gauge, load_sem.at[1])
    source_load.start()
    gauge_load.start()
    barrier = pltpu.get_barrier_semaphore()
    for target in targets:
        pl.semaphore_signal(barrier, inc=1, device_id=target, device_id_type=MESH)

    upper = (2 * gz) // nz
    early, late = 2 + upper, 3 - upper
    early_sign = (1 - 2 * upper).astype(jnp.float32)

    def halo_copy(step, halo, g):
        if isinstance(halo, int):
            target = targets[halo]
        else:
            target = (ta, lax.rem(gz + (3 - halo) * (nz - 1) + (halo - 2), nz))
        return pltpu.make_async_remote_copy(
            src_ref=sent.at[step, halo, g],
            dst_ref=got.at[step, halo, g],
            send_sem=send_sem.at[step, halo, g],
            recv_sem=recv_sem.at[step, halo, g],
            device_id=target,
            device_id_type=MESH,
        )

    def link_copy(which):
        return pltpu.make_async_remote_copy(
            src_ref=gauge_hbm.at[pl.ds(9 * (3 - which), 9)],
            dst_ref=links_below.at[which],
            send_sem=link_send.at[which],
            recv_sem=link_recv.at[which],
            device_id=(above_t, above_z)[which],
            device_id_type=MESH,
        )

    def put_halos(step, g, at):
        for halo, (direction, hop_sign) in enumerate(HALOS):
            half = project(at, direction, hop_sign)
            for s in range(2):
                for c in range(3):
                    sent[step, halo, g, pl.ds((s * 3 + c) * 16, 16)] = half[s][c]

    def rows_of(ri, s, c, g):
        return pl.ds(((ri * 3 + c) * groups + g) * 32 + s, 8, stride=4)

    source_load.wait()
    for p in range(source.shape[0]):
        wide[8 * p : 8 * p + 8] = source[p].astype(jnp.float32)
    for g in range(groups):
        for ri in range(2):
            for s in range(4):
                for c in range(3):
                    psi[0, g, plane(ri, s, c)] = wide[rows_of(ri, s, c, g)]

    def load_psi(step, g):
        return lambda ri, s, c: psi[step, g, plane(ri, s, c)]

    def first_halos(g, carry):
        put_halos(0, g, load_psi(0, g))
        return carry

    lax.fori_loop(0, groups, first_halos, 0)
    pl.semaphore_wait(barrier, 4)
    for which in range(2):
        link_copy(which).start()

    def first_sends(g, carry):
        for halo in (0, 1, late):
            halo_copy(0, halo, g).start()
        return carry

    for g in range(groups):
        halo_copy(0, early, g).start()
    lax.fori_loop(0, groups, first_sends, 0)

    first_half = lax.broadcasted_iota(jnp.int32, (8, LANES), 0) % 2 == 0

    def spread(rows, ri, scale):
        return scale * jnp.where(
            first_half,
            jnp.broadcast_to(rows[ri : ri + 1], (8, LANES)),
            jnp.broadcast_to(rows[2 + ri : 3 + ri], (8, LANES)),
        )

    def put_link(direction, hop_sign, ri, r, c, tile):
        if hop_sign > 0:
            links[link_slot(direction, 1), ri * 9 + r * 3 + c] = tile
        else:
            links[link_slot(direction, -1), ri * 9 + c * 3 + r] = tile if ri == 0 else -tile

    forward_scale = jnp.where(ta == nt - 1, HOPPING, -HOPPING).astype(jnp.float32)
    backward_scale = jnp.where(ta == 0, HOPPING, -HOPPING).astype(jnp.float32)
    gauge_load.wait()
    for direction in range(4):
        scale = forward_scale if direction == 3 else jnp.float32(-HOPPING)
        for r in range(3):
            for c in range(3):
                rows = gauge[direction * 9 + r * 3 + c].astype(jnp.float32)
                for ri in range(2):
                    tile = spread(rows, ri, scale)
                    put_link(direction, 1, ri, r, c, tile)
                    if direction < 2:
                        put_link(direction, -1, ri, r, c, shift_sites(tile, direction, -1))

    def load_link(direction, hop_sign):
        slot = link_slot(direction, hop_sign)
        return lambda ri, r, c: links[slot, ri * 9 + r * 3 + c]

    def load_spinor(at):
        return [[[at(ri, s, c) for c in range(3)] for s in range(4)] for ri in range(2)]

    def plane_hops(step):
        def body(g, carry):
            at = load_psi(step, g)
            total = load_spinor(at)
            for direction in (0, 1):
                for hop_sign in (1, -1):
                    pairs = project(at, direction, hop_sign)
                    half = [
                        [
                            tuple(shift_sites(v, direction, hop_sign) for v in widened(pairs[s][c]))
                            for c in range(3)
                        ]
                        for s in range(2)
                    ]
                    add_hop(total, half, load_link(direction, hop_sign), direction, hop_sign)
            for ri in range(2):
                for s in range(4):
                    for c in range(3):
                        acc[g, plane(ri, s, c)] = total[ri][s][c]
            return carry

        lax.fori_loop(0, groups, body, 0)

    def add_halo(total, step, halo, g, link, direction, hop_sign):
        halo_copy(step, halo, g).wait_recv()
        half = [
            [widened(got[step, halo, g, pl.ds((s * 3 + c) * 16, 16)]) for c in range(3)]
            for s in range(2)
        ]
        add_hop(total, half, link, direction, hop_sign)

    def slot_link(slot):
        return lambda ri, r, c: links[slot, ri * 9 + r * 3 + c]

    def early_hops(g, carry):
        total = load_spinor(lambda ri, s, c: acc[g, plane(ri, s, c)])
        for halo, (direction, hop_sign) in enumerate(HALOS[:2]):
            add_halo(total, 0, halo, g, load_link(direction, hop_sign), direction, hop_sign)
        add_halo(total, 0, early, g, slot_link(4 + upper), 2, early_sign)
        half = project(lambda ri, s, c: total[ri][s][c], 2, early_sign)
        for s in range(2):
            for c in range(3):
                sent[1, early, g, pl.ds((s * 3 + c) * 16, 16)] = half[s][c]
        for ri in range(2):
            for s in range(4):
                for c in range(3):
                    acc[g, plane(ri, s, c)] = total[ri][s][c]
        halo_copy(1, early, g).start()
        return carry

    def halo_hops(step):
        def body(g, carry):
            total = load_spinor(lambda ri, s, c: acc[g, plane(ri, s, c)])
            if step == 0:
                add_halo(total, 0, late, g, slot_link(5 - upper), 2, -early_sign)
            else:
                for halo, (direction, hop_sign) in enumerate(HALOS):
                    add_halo(total, 1, halo, g, load_link(direction, hop_sign), direction, hop_sign)
            final = {}
            for s in range(4):
                for c in range(3):
                    final[0, s, c], final[1, s, c] = widened(
                        rounded(total[0][s][c], total[1][s][c])
                    )
            for (ri, s, c), tile in final.items():
                if step == 0:
                    psi[1, g, plane(ri, s, c)] = tile
                else:
                    wide[rows_of(ri, s, c, g)] = tile
            if step == 0:
                at = lambda ri, s, c: final[ri, s, c]
                halves = (
                    (0, project(at, 3, 1)), (1, project(at, 3, -1)), (late, project(at, 2, -early_sign))
                )
                for halo, half in halves:
                    for s in range(2):
                        for c in range(3):
                            sent[1, halo, g, pl.ds((s * 3 + c) * 16, 16)] = half[s][c]
                for halo, _ in halves:
                    halo_copy(1, halo, g).start()
            else:
                for block in range(6):
                    for p in range(4):
                        at = (block * groups + g) * 4 + p
                        out[at] = wide[pl.ds(8 * at, 8)].astype(jnp.bfloat16)
            return carry

        lax.fori_loop(0, groups, body, 0)

    plane_hops(0)
    for which, scale in ((0, backward_scale), (1, jnp.float32(-HOPPING))):
        link_copy(which).wait_recv()
        for r in range(3):
            for c in range(3):
                rows = links_below[which, r * 3 + c].astype(jnp.float32)
                for ri in range(2):
                    put_link(3 - which, -1, ri, r, c, spread(rows, ri, scale))
    lax.fori_loop(0, groups, early_hops, 0)
    halo_hops(0)
    plane_hops(1)
    halo_hops(1)

    def drain(g, carry):
        for step in range(2):
            for halo in range(4):
                halo_copy(step, halo, g).wait_send()
        return carry

    lax.fori_loop(0, groups, drain, 0)
    for which in range(2):
        link_copy(which).wait_send()


def body(source, gauge_field):
    rhs = source.shape[5]
    groups = rhs // 4
    source_rows = source.reshape(2, 4, 3, rhs, 2, LANES).transpose(0, 2, 3, 4, 1, 5)
    source_rows = source_rows.reshape(6 * rhs, 8, LANES)
    gauge_rows = gauge_field.reshape(4, 2, 3, 3, 2, LANES).transpose(0, 2, 3, 4, 1, 5)
    gauge_rows = gauge_rows.reshape(36, 4, LANES)
    rows = pl.pallas_call(
        functools.partial(kernel, groups),
        out_shape=pltpu.VMEM(source_rows.shape, source.dtype),
        in_specs=[pl.BlockSpec(memory_space=pltpu.HBM)] * 2,
        out_specs=pl.BlockSpec(memory_space=pltpu.VMEM),
        scratch_shapes=[
            pltpu.VMEM(source_rows.shape, jnp.bfloat16),
            pltpu.VMEM(gauge_rows.shape, jnp.bfloat16),
            pltpu.VMEM((48 * rhs, LANES), jnp.float32),
            pltpu.VMEM((2, groups, 24, 8, LANES), jnp.float32),
            pltpu.VMEM((groups, 24, 8, LANES), jnp.float32),
            pltpu.VMEM((8, 18, 8, LANES), jnp.float32),
            pltpu.VMEM((2, 4, groups, 96, LANES), jnp.bfloat16),
            pltpu.VMEM((2, 4, groups, 96, LANES), jnp.bfloat16),
            pltpu.VMEM((2, 9, 4, LANES), jnp.bfloat16),
            pltpu.SemaphoreType.DMA((2,)),
            pltpu.SemaphoreType.DMA((2, 4, groups)),
            pltpu.SemaphoreType.DMA((2, 4, groups)),
            pltpu.SemaphoreType.DMA((2,)),
            pltpu.SemaphoreType.DMA((2,)),
        ],
        compiler_params=pltpu.CompilerParams(collective_id=0, has_side_effects=True),
        name="dirac_twice",
    )(source_rows, gauge_rows)
    out = rows.reshape(2, 3, rhs, 2, 4, LANES).transpose(0, 4, 1, 2, 3, 5)
    return out.reshape(source.shape)


def solution(mesh):
    spec = P("ta", "gz", None, None, None, None, None)
    return jax.shard_map(body, mesh=mesh, in_specs=(spec, spec), out_specs=spec, check_vma=False)
```

```python
import functools

import jax
import jax.numpy as jnp
from jax import lax
from jax.experimental import pallas as pl
from jax.experimental.pallas import tpu as pltpu
from jax.sharding import PartitionSpec as P

NX = 16
HOPPING = 0.124
GAMMA_PERM = ((3, 2, 1, 0), (3, 2, 1, 0), (2, 3, 0, 1), (2, 3, 0, 1))
GAMMA_PHASE = (
    ((0, 1), (0, 1), (0, -1), (0, -1)),
    ((-1, 0), (1, 0), (1, 0), (-1, 0)),
    ((0, 1), (0, -1), (0, -1), (0, 1)),
    ((1, 0), (1, 0), (1, 0), (1, 0)),
)
LANES = 128
MESH = pl.DeviceIdType.MESH

HALOS = ((3, 1), (3, -1), (2, 1), (2, -1))


def signed_sum(base, term, sign):
    if not isinstance(sign, int):
        return base + term * sign
    return base + term if sign > 0 else base - term


def rounded(first, second):
    return jnp.concatenate([first, second], 0).astype(jnp.bfloat16)


def project(psi, direction, hop_sign):
    out = []
    for s in range(2):
        partner = GAMMA_PERM[direction][s]
        pr, pi = GAMMA_PHASE[direction][s]
        row = []
        for c in range(3):
            if pi == 0:
                re = signed_sum(psi(0, s, c), psi(0, partner, c), -hop_sign * pr)
                im = signed_sum(psi(1, s, c), psi(1, partner, c), -hop_sign * pr)
            else:
                re = signed_sum(psi(0, s, c), psi(1, partner, c), hop_sign * pi)
                im = signed_sum(psi(1, s, c), psi(0, partner, c), -hop_sign * pi)
            row.append(rounded(re, im))
        out.append(row)
    return out


def widened(pair):
    wide = pair.astype(jnp.float32)
    return wide[:8], wide[8:]


def shift_sites(tile, direction, steps):
    lane = lax.broadcasted_iota(jnp.int32, (8, LANES), 1)
    if direction == 0:
        column = lane % NX
        if steps > 0:
            return jnp.where(
                column == NX - 1,
                pltpu.roll(tile, NX - 1, axis=1),
                pltpu.roll(tile, LANES - 1, axis=1),
            )
        return jnp.where(
            column == 0,
            pltpu.roll(tile, LANES - (NX - 1), axis=1),
            pltpu.roll(tile, 1, axis=1),
        )
    near = pltpu.roll(tile, LANES - NX if steps > 0 else NX, axis=1)
    first_half = lax.broadcasted_iota(jnp.int32, (8, LANES), 0) % 2 == 0
    other = jnp.where(first_half, pltpu.roll(near, 7, axis=0), pltpu.roll(near, 1, axis=0))
    return jnp.where(lane >= LANES - NX if steps > 0 else lane < NX, other, near)


def add_hop(acc, half, link, direction, hop_sign):
    for r in range(3):
        lr = [link(0, r, c) for c in range(3)]
        li = [link(1, r, c) for c in range(3)]
        k = []
        for s in range(2):
            re = im = None
            for c in range(3):
                hr, hi = half[s][c]
                tr = lr[c] * hr - li[c] * hi
                ti = lr[c] * hi + li[c] * hr
                re = tr if re is None else re + tr
                im = ti if im is None else im + ti
            k.append((re, im))
            acc[0][s][r] = acc[0][s][r] + re
            acc[1][s][r] = acc[1][s][r] + im
        for s in (2, 3):
            kr, ki = k[GAMMA_PERM[direction][s]]
            pr, pi = GAMMA_PHASE[direction][s]
            if pi == 0:
                acc[0][s][r] = signed_sum(acc[0][s][r], kr, -hop_sign * pr)
                acc[1][s][r] = signed_sum(acc[1][s][r], ki, -hop_sign * pr)
            else:
                acc[0][s][r] = signed_sum(acc[0][s][r], ki, hop_sign * pi)
                acc[1][s][r] = signed_sum(acc[1][s][r], kr, -hop_sign * pi)


def plane(ri, s, c):
    return (ri * 4 + s) * 3 + c


def link_slot(direction, hop_sign):
    return direction * 2 + (0 if hop_sign > 0 else 1)


def kernel(
    groups, source_hbm, gauge_hbm, out, source, gauge, wide, psi, acc, links, sent, got,
    links_below, load_sem, send_sem, recv_sem, link_send, link_recv,
):
    ta, gz = lax.axis_index("ta"), lax.axis_index("gz")
    nt, nz = lax.axis_size("ta"), lax.axis_size("gz")
    above_t = (lax.rem(ta + 1, nt), gz)
    below_t = (lax.rem(ta + nt - 1, nt), gz)
    above_z = (ta, lax.rem(gz + 1, nz))
    below_z = (ta, lax.rem(gz + nz - 1, nz))
    targets = (below_t, above_t, below_z, above_z)

    source_load = pltpu.make_async_copy(source_hbm, source, load_sem.at[0])
    gauge_load = pltpu.make_async_copy(gauge_hbm, gauge, load_sem.at[1])
    source_load.start()
    gauge_load.start()
    barrier = pltpu.get_barrier_semaphore()
    for target in targets:
        pl.semaphore_signal(barrier, inc=1, device_id=target, device_id_type=MESH)

    upper = (2 * gz) // nz
    early, late = 2 + upper, 3 - upper
    early_sign = (1 - 2 * upper).astype(jnp.float32)

    def halo_copy(step, halo, g):
        if isinstance(halo, int):
            target = targets[halo]
        else:
            target = (ta, lax.rem(gz + (3 - halo) * (nz - 1) + (halo - 2), nz))
        return pltpu.make_async_remote_copy(
            src_ref=sent.at[step, halo, g],
            dst_ref=got.at[step, halo, g],
            send_sem=send_sem.at[step, halo, g],
            recv_sem=recv_sem.at[step, halo, g],
            device_id=target,
            device_id_type=MESH,
        )

    def link_copy(which):
        return pltpu.make_async_remote_copy(
            src_ref=gauge.at[pl.ds(9 * (3 - which), 9)],
            dst_ref=links_below.at[which],
            send_sem=link_send.at[which],
            recv_sem=link_recv.at[which],
            device_id=(above_t, above_z)[which],
            device_id_type=MESH,
        )

    def put_halos(step, g, at):
        for halo, (direction, hop_sign) in enumerate(HALOS):
            half = project(at, direction, hop_sign)
            for s in range(2):
                for c in range(3):
                    sent[step, halo, g, pl.ds((s * 3 + c) * 16, 16)] = half[s][c]

    def rows_of(ri, s, c, g):
        return pl.ds(((ri * 3 + c) * groups + g) * 32 + s, 8, stride=4)

    source_load.wait()
    for p in range(source.shape[0]):
        wide[8 * p : 8 * p + 8] = source[p].astype(jnp.float32)
    for g in range(groups):
        for ri in range(2):
            for s in range(4):
                for c in range(3):
                    psi[0, g, plane(ri, s, c)] = wide[rows_of(ri, s, c, g)]

    def load_psi(step, g):
        return lambda ri, s, c: psi[step, g, plane(ri, s, c)]

    def first_halos(g, carry):
        put_halos(0, g, load_psi(0, g))
        return carry

    lax.fori_loop(0, groups, first_halos, 0)
    gauge_load.wait()
    pl.semaphore_wait(barrier, 4)

    def first_sends(g, carry):
        for halo in (0, 1, late):
            halo_copy(0, halo, g).start()
        return carry

    halo_copy(0, early, 0).start()
    for which in range(2):
        link_copy(which).start()
    for g in range(1, groups):
        halo_copy(0, early, g).start()
    lax.fori_loop(0, groups, first_sends, 0)

    first_half = lax.broadcasted_iota(jnp.int32, (8, LANES), 0) % 2 == 0

    def spread(rows, ri, scale):
        return scale * jnp.where(
            first_half,
            jnp.broadcast_to(rows[ri : ri + 1], (8, LANES)),
            jnp.broadcast_to(rows[2 + ri : 3 + ri], (8, LANES)),
        )

    def put_link(direction, hop_sign, ri, r, c, tile):
        if hop_sign > 0:
            links[link_slot(direction, 1), ri * 9 + r * 3 + c] = tile
        else:
            links[link_slot(direction, -1), ri * 9 + c * 3 + r] = tile if ri == 0 else -tile

    forward_scale = jnp.where(ta == nt - 1, HOPPING, -HOPPING).astype(jnp.float32)
    backward_scale = jnp.where(ta == 0, HOPPING, -HOPPING).astype(jnp.float32)
    for direction in range(4):
        scale = forward_scale if direction == 3 else jnp.float32(-HOPPING)
        for r in range(3):
            for c in range(3):
                rows = gauge[direction * 9 + r * 3 + c].astype(jnp.float32)
                for ri in range(2):
                    tile = spread(rows, ri, scale)
                    put_link(direction, 1, ri, r, c, tile)
                    if direction < 2:
                        put_link(direction, -1, ri, r, c, shift_sites(tile, direction, -1))

    def load_link(direction, hop_sign):
        slot = link_slot(direction, hop_sign)
        return lambda ri, r, c: links[slot, ri * 9 + r * 3 + c]

    def load_spinor(at):
        return [[[at(ri, s, c) for c in range(3)] for s in range(4)] for ri in range(2)]

    def plane_hops(step):
        def body(g, carry):
            at = load_psi(step, g)
            total = load_spinor(at)
            for direction in (0, 1):
                for hop_sign in (1, -1):
                    pairs = project(at, direction, hop_sign)
                    half = [
                        [
                            tuple(shift_sites(v, direction, hop_sign) for v in widened(pairs[s][c]))
                            for c in range(3)
                        ]
                        for s in range(2)
                    ]
                    add_hop(total, half, load_link(direction, hop_sign), direction, hop_sign)
            for ri in range(2):
                for s in range(4):
                    for c in range(3):
                        acc[g, plane(ri, s, c)] = total[ri][s][c]
            return carry

        lax.fori_loop(0, groups, body, 0)

    def add_halo(total, step, halo, g, link, direction, hop_sign):
        halo_copy(step, halo, g).wait_recv()
        half = [
            [widened(got[step, halo, g, pl.ds((s * 3 + c) * 16, 16)]) for c in range(3)]
            for s in range(2)
        ]
        add_hop(total, half, link, direction, hop_sign)

    def slot_link(slot):
        return lambda ri, r, c: links[slot, ri * 9 + r * 3 + c]

    def early_hops(g, carry):
        total = load_spinor(lambda ri, s, c: acc[g, plane(ri, s, c)])
        for halo, (direction, hop_sign) in enumerate(HALOS[:2]):
            add_halo(total, 0, halo, g, load_link(direction, hop_sign), direction, hop_sign)
        add_halo(total, 0, early, g, slot_link(4 + upper), 2, early_sign)
        half = project(lambda ri, s, c: total[ri][s][c], 2, early_sign)
        for s in range(2):
            for c in range(3):
                sent[1, early, g, pl.ds((s * 3 + c) * 16, 16)] = half[s][c]
        for ri in range(2):
            for s in range(4):
                for c in range(3):
                    acc[g, plane(ri, s, c)] = total[ri][s][c]
        halo_copy(1, early, g).start()
        return carry

    def halo_hops(step):
        def body(g, carry):
            total = load_spinor(lambda ri, s, c: acc[g, plane(ri, s, c)])
            if step == 0:
                add_halo(total, 0, late, g, slot_link(5 - upper), 2, -early_sign)
            else:
                for halo, (direction, hop_sign) in enumerate(HALOS):
                    add_halo(total, 1, halo, g, load_link(direction, hop_sign), direction, hop_sign)
            final = {}
            for s in range(4):
                for c in range(3):
                    final[0, s, c], final[1, s, c] = widened(
                        rounded(total[0][s][c], total[1][s][c])
                    )
            for (ri, s, c), tile in final.items():
                if step == 0:
                    psi[1, g, plane(ri, s, c)] = tile
                else:
                    wide[rows_of(ri, s, c, g)] = tile
            if step == 0:
                at = lambda ri, s, c: final[ri, s, c]
                halves = (
                    (0, project(at, 3, 1)), (1, project(at, 3, -1)), (late, project(at, 2, -early_sign))
                )
                for halo, half in halves:
                    for s in range(2):
                        for c in range(3):
                            sent[1, halo, g, pl.ds((s * 3 + c) * 16, 16)] = half[s][c]
                for halo, _ in halves:
                    halo_copy(1, halo, g).start()
            else:
                for block in range(6):
                    for p in range(4):
                        at = (block * groups + g) * 4 + p
                        out[at] = wide[pl.ds(8 * at, 8)].astype(jnp.bfloat16)
            return carry

        lax.fori_loop(0, groups, body, 0)

    plane_hops(0)
    def take_links(which, scale):
        link_copy(which).wait_recv()
        for r in range(3):
            for c in range(3):
                rows = links_below[which, r * 3 + c].astype(jnp.float32)
                for ri in range(2):
                    put_link(3 - which, -1, ri, r, c, spread(rows, ri, scale))
    take_links(0, backward_scale)
    pl.when(upper == 1)(lambda: take_links(1, jnp.float32(-HOPPING)))
    lax.fori_loop(0, groups, early_hops, 0)
    pl.when(upper == 0)(lambda: take_links(1, jnp.float32(-HOPPING)))
    halo_hops(0)
    plane_hops(1)
    halo_hops(1)

    def drain(g, carry):
        for step in range(2):
            for halo in range(4):
                halo_copy(step, halo, g).wait_send()
        return carry

    lax.fori_loop(0, groups, drain, 0)
    for which in range(2):
        link_copy(which).wait_send()


def body(source, gauge_field):
    rhs = source.shape[5]
    groups = rhs // 4
    source_rows = source.reshape(2, 4, 3, rhs, 2, LANES).transpose(0, 2, 3, 4, 1, 5)
    source_rows = source_rows.reshape(6 * rhs, 8, LANES)
    gauge_rows = gauge_field.reshape(4, 2, 3, 3, 2, LANES).transpose(0, 2, 3, 4, 1, 5)
    gauge_rows = gauge_rows.reshape(36, 4, LANES)
    rows = pl.pallas_call(
        functools.partial(kernel, groups),
        out_shape=pltpu.VMEM(source_rows.shape, source.dtype),
        in_specs=[pl.BlockSpec(memory_space=pltpu.HBM)] * 2,
        out_specs=pl.BlockSpec(memory_space=pltpu.VMEM),
        scratch_shapes=[
            pltpu.VMEM(source_rows.shape, jnp.bfloat16),
            pltpu.VMEM(gauge_rows.shape, jnp.bfloat16),
            pltpu.VMEM((48 * rhs, LANES), jnp.float32),
            pltpu.VMEM((2, groups, 24, 8, LANES), jnp.float32),
            pltpu.VMEM((groups, 24, 8, LANES), jnp.float32),
            pltpu.VMEM((8, 18, 8, LANES), jnp.float32),
            pltpu.VMEM((2, 4, groups, 96, LANES), jnp.bfloat16),
            pltpu.VMEM((2, 4, groups, 96, LANES), jnp.bfloat16),
            pltpu.VMEM((2, 9, 4, LANES), jnp.bfloat16),
            pltpu.SemaphoreType.DMA((2,)),
            pltpu.SemaphoreType.DMA((2, 4, groups)),
            pltpu.SemaphoreType.DMA((2, 4, groups)),
            pltpu.SemaphoreType.DMA((2,)),
            pltpu.SemaphoreType.DMA((2,)),
        ],
        compiler_params=pltpu.CompilerParams(collective_id=0, has_side_effects=True),
        name="dirac_twice",
    )(source_rows, gauge_rows)
    out = rows.reshape(2, 3, rhs, 2, 4, LANES).transpose(0, 4, 1, 2, 3, 5)
    return out.reshape(source.shape)


def solution(mesh):
    spec = P("ta", "gz", None, None, None, None, None)
    return jax.shard_map(body, mesh=mesh, in_specs=(spec, spec), out_specs=spec, check_vma=False)
```
